256 devices in a mesh: slab: 128 (over x, z, y), pencil: 2 (over core).
Axes of the slice: x: 4, y: 4, z: 8, core: 2. Of those that a mesh axis runs over, the one named last changes fastest.
Arguments:
- density: float32 [768, 768, 384], P('slab', 'pencil'), may hold values from 0 to 1
- cell_kind: int32 [768, 768, 384], P('slab', 'pencil'), may hold values from 0 to 2
- sharpness: float32 [1], replicated, may hold values from 48 to 96
- fraction: float32 [1], replicated, may hold values from 0.36 to 0.41
Outputs:
- physical: float32 [768, 768, 384], P('slab', 'pencil')
- threshold: float32 [1], replicated
The draws below stay inside these ranges and needn't reach their ends.
Inputs may be any that keep to these rules, and one draw needn't show every extreme that they name: `cell_kind`: each cell is a design, void or solid cell.
All inputs are finite; a program needn't handle non-finite values.
Results may differ from the reference program's by a relative error of at most 0.0003.
Values sent between devices are 32-bit elements; how exact they have to be, the bound alone decides.
A program may use at most 128 MiB of HBM per device.

```python
import math
import jax
import jax.numpy as jnp
from jax import lax

RADIUS = 5
ITERS = 3
NZ = 768
NY = 768
NX = 384


def draw_density(key, part):
    wave_draw = jax.random.uniform(jax.random.fold_in(key, 11), (6, 3), jnp.float32)
    sign_flip = jnp.where(jax.random.bernoulli(jax.random.fold_in(key, 12), 0.5, (6, 3)), 1.0, -1.0)
    phase_shift = jax.random.uniform(jax.random.fold_in(key, 13), (6,), jnp.float32, -math.pi, math.pi)
    cycles = sign_flip / (24.0 * jnp.power(4.0, wave_draw))
    depth_axis = jnp.arange(NZ, dtype=jnp.float32)[:, None, None]
    row_axis = jnp.arange(NY, dtype=jnp.float32)[None, :, None]
    column_axis = jnp.arange(NX, dtype=jnp.float32)[None, None, :]
    pattern = jnp.zeros((NZ, NY, NX), jnp.float32)
    for component in range(6):
        argument = cycles[component, 0] * depth_axis + cycles[component, 1] * row_axis + cycles[component, 2] * column_axis
        pattern = pattern + jnp.cos(2.0 * math.pi * argument + phase_shift[component])
    pattern = pattern / math.sqrt(3.0)
    middle_value = 0.62
    amplitude = 0.3
    roughness = 0.2
    jitter = jax.random.uniform(jax.random.fold_in(key, 14), (NZ, NY, NX), jnp.float32, -roughness, roughness)
    return jnp.clip(middle_value + amplitude * pattern + jitter, 0.0, 1.0).astype(jnp.float32)


def set_ends(result, stream_key, low, largest):
    dims = result.shape
    place = [jax.random.randint(jax.random.fold_in(stream_key, axis), (), 0, dims[axis]) for axis in range(len(dims))]
    result = result.at[tuple(place)].set(low)
    longest = dims.index(max(dims))
    place[longest] = (place[longest] + 1) % dims[longest]
    return result.at[tuple(place)].set(largest)


def setup_inputs(seed: int = 0) -> dict:
    key_list = jax.random.split(jax.random.key(seed), 5)
    density = draw_density(jax.random.fold_in(key_list[4], 71), 0)
    cell_kind = set_ends(jax.random.randint(key_list[1], (NZ, NY, NX), 0, 3), jax.random.fold_in(key_list[1], 1), 0, 2).astype(jnp.int32)
    sharpness = jnp.clip(jnp.exp(jax.random.uniform(key_list[2], (1,), jnp.float32, math.log(48.0), math.log(96.0))), 48.0, 96.0)
    fraction = jnp.clip(jax.random.uniform(key_list[3], (1,), jnp.float32, 0.36, 0.41), 0.36, 0.41)
    return dict(density=density, cell_kind=cell_kind, sharpness=sharpness, fraction=fraction)


def smooth_axis(field, axis):
    length = field.shape[axis]
    pads = [(0, 0), (0, 0), (0, 0)]
    pads[axis] = (RADIUS, RADIUS)
    padded = jnp.pad(field, pads)
    total = jnp.zeros_like(field)
    for offset in range(-RADIUS, RADIUS + 1):
        weight = float(RADIUS + 1 - abs(offset))
        piece = lax.slice_in_dim(padded, RADIUS + offset, RADIUS + offset + length, axis=axis)
        total = total + weight * piece
    return total


def coverage(count):
    index = jnp.arange(count, dtype=jnp.int32)
    total = jnp.zeros((count,), jnp.float32)
    for offset in range(-RADIUS, RADIUS + 1):
        inside = ((index + offset >= 0) & (index + offset < count)).astype(jnp.float32)
        total = total + float(RADIUS + 1 - abs(offset)) * inside
    return total


def project(filtered, cell_kind, beta, level):
    tangent = jnp.tanh(beta * (filtered - level))
    design = cell_kind == 0
    solid = cell_kind == 2
    values = jnp.where(design, 0.5 * (1.0 + tangent), jnp.where(solid, 1.0, 0.0))
    return values, tangent, design


def reference(density, cell_kind, sharpness, fraction):
    smoothed = smooth_axis(smooth_axis(smooth_axis(density, 0), 1), 2)
    cover = coverage(NZ)[:, None, None] * coverage(NY)[None, :, None] * coverage(NX)[None, None, :]
    filtered = smoothed / cover
    beta = sharpness[0]
    cells = jnp.float32(NZ * NY * NX)
    level = jnp.float32(0.5)
    for step in range(ITERS):
        values, tangent, design = project(filtered, cell_kind, beta, level)
        volume = jnp.sum(values)
        slope = cells + jnp.sum(jnp.where(design, 0.5 * beta * (1.0 - tangent * tangent), 0.0))
        level = level + (volume - fraction[0] * cells) / slope
    values, tangent, design = project(filtered, cell_kind, beta, level)
    return values, jnp.reshape(level, (1,)).astype(jnp.float32)
```

```python
import functools

import jax
import jax.numpy as jnp
from jax import lax
from jax.experimental import pallas as pl
from jax.experimental.pallas import tpu as pltpu
from jax.sharding import PartitionSpec as P

RADIUS = 5
ITERS = 3
CHUNK = 16
PAD = 8
WINDOW = 6
LANES = 128
FAR = 1.0e6
MESH = pl.DeviceIdType.MESH


def box(values):
    pairs = [a + b for a, b in zip(values[:-1], values[1:])]
    return [pairs[k] + pairs[k + 2] + pairs[k + 4] for k in range(len(values) - RADIUS)]


def triangle(k):
    k = jnp.maximum(k, 0)
    return (k * (k + 1)) // 2


def coverage(index, whole):
    full = (RADIUS + 1) * (RADIUS + 1)
    return (full - triangle(RADIUS - index) - triangle(RADIUS + 1 + index - whole)).astype(jnp.float32)


def split(x):
    high = x.astype(jnp.bfloat16)
    return high, (x - high.astype(jnp.float32)).astype(jnp.bfloat16)


def band(shape, shift):
    row = lax.broadcasted_iota(jnp.int32, shape, 0)
    col = lax.broadcasted_iota(jnp.int32, shape, 1)
    return jnp.maximum(RADIUS + 1 - jnp.abs(col - shift - row), 0).astype(jnp.float32).astype(jnp.bfloat16)


def folded(x):
    tiles = [
        x[i : i + 8, j : j + LANES] for i in range(0, x.shape[0], 8) for j in range(0, x.shape[1], LANES)
    ]
    while len(tiles) > 1:
        tiles = [sum(tiles[i : i + 2][1:], tiles[i]) for i in range(0, len(tiles), 2)]
    return tiles[0]


def kernel(slabs, pencils, beta_ref, fraction_ref, density, kind, coded, level_out, own, below, above, kinds,
           along_z, x_band, acc, parts, u_send, u_recv, d_send, d_recv, h_send, h_recv, local_sem, r_send, r_recv):
    depth, rows, cols = density.shape
    steps = rows // CHUNK
    slab = lax.axis_index("slab")
    pencil = lax.axis_index("pencil")
    first = pencil == 0
    devices = slabs * pencils
    me = slab * pencils + pencil

    barrier = pltpu.get_barrier_semaphore()

    def greet(k, carry):
        there = slab + (slabs - k)
        there = there - jnp.where(there >= slabs, slabs, 0)
        for core in range(pencils):
            pl.semaphore_signal(barrier, inc=1, device_id=(there, core), device_id_type=MESH)
        return carry

    lax.fori_loop(1, slabs, greet, 0, unroll=15 if slabs % 15 == 1 else 1)
    pl.semaphore_signal(barrier, inc=1, device_id=(slab, 1 - pencil), device_id_type=MESH)

    has_above = slab + 1 < slabs
    has_below = slab > 0
    upper = jnp.minimum(slab + 1, slabs - 1)
    lower = jnp.maximum(slab - 1, 0)
    sibling = 1 - pencil
    halo = pl.multiple_of(jnp.where(first, PAD + rows, 0), 8)
    edge = pl.multiple_of(jnp.where(first, 0, PAD + rows), 8)
    there = pl.multiple_of(jnp.where(first, 0, PAD + rows), 8)
    mine = pl.multiple_of(jnp.where(first, rows, PAD), 8)

    def row_of(k):
        return pl.multiple_of(jnp.where(first, steps - 1 - k, k) * CHUNK, CHUNK)

    def up_copy(k):
        r = row_of(k)
        return pltpu.make_async_remote_copy(
            density.at[pl.ds(depth - RADIUS, RADIUS), pl.ds(r, CHUNK), :], below.at[:, pl.ds(r + PAD, CHUNK), :],
            u_send.at[k], u_recv.at[k], device_id=(upper, pencil), device_id_type=MESH)

    def down_copy(k):
        r = row_of(k)
        return pltpu.make_async_remote_copy(
            density.at[pl.ds(0, RADIUS), pl.ds(r, CHUNK), :], above.at[:, pl.ds(r + PAD, CHUNK), :],
            d_send.at[k], d_recv.at[k], device_id=(lower, pencil), device_id_type=MESH)

    def halo_copy(index, src, dst):
        return pltpu.make_async_remote_copy(
            src, dst, h_send.at[index], h_recv.at[index], device_id=(slab, sibling), device_id_type=MESH)

    own_row = pl.multiple_of(jnp.where(first, rows - PAD, 0), 8)
    own_halo = halo_copy(0, density.at[:, pl.ds(own_row, PAD), :], own.at[:, pl.ds(there, PAD), :])
    below_halo = halo_copy(1, below.at[:, pl.ds(mine, PAD), :], below.at[:, pl.ds(there, PAD), :])
    above_halo = halo_copy(2, above.at[:, pl.ds(mine, PAD), :], above.at[:, pl.ds(there, PAD), :])
    own_load = pltpu.make_async_copy(density, own.at[:, pl.ds(PAD, rows), :], local_sem.at[0])
    kind_load = pltpu.make_async_copy(kind, kinds, local_sem.at[1])

    own_load.start()
    kind_load.start()
    pl.semaphore_wait(barrier, devices - 1)

    def send_chunk(k):
        @pl.when(has_above)
        def _():
            up_copy(k).start()

        @pl.when(has_below)
        def _():
            down_copy(k).start()

    for k in range(min(WINDOW, steps)):
        send_chunk(k)
    own_halo.start()

    x_band[...] = band((cols, cols), 0)
    acc[...] = jnp.zeros_like(acc)
    along_z[:, pl.ds(edge, PAD), :] = jnp.zeros((depth, PAD, cols), jnp.float32)

    @pl.when(jnp.logical_not(has_below))
    def _():
        @pl.loop(0, RADIUS)
        def _(k):
            below[k] = jnp.zeros(below.shape[1:], jnp.float32)

    @pl.when(jnp.logical_not(has_above))
    def _():
        @pl.loop(0, RADIUS)
        def _(k):
            above[k] = jnp.zeros(above.shape[1:], jnp.float32)

    beta = beta_ref[0]

    def filter_z(start, count):
        for r in range(0, count, 8):
            for c in range(0, cols, LANES):
                at = (pl.ds(pl.multiple_of(start + r, 8), 8), pl.ds(c, LANES))
                values = [below[m, at[0], at[1]] for m in range(RADIUS)]
                values += [own[i, at[0], at[1]] for i in range(depth)]
                values += [above[i, at[0], at[1]] for i in range(RADIUS)]
                for i, out in enumerate(box(box(values))):
                    along_z[i, at[0], at[1]] = out

    def filter_yx(j):
        r = row_of(j)
        y_band = band((CHUNK, CHUNK + 2 * PAD), PAD)
        pieces = []
        for layer in range(depth):
            high, low = split(along_z[layer, pl.ds(r, CHUNK + 2 * PAD), :])
            pieces.append(jnp.dot(y_band, high, preferred_element_type=jnp.float32)
                          + jnp.dot(y_band, low, preferred_element_type=jnp.float32))
        high, low = split(jnp.concatenate(pieces, axis=0))
        smoothed = (jnp.dot(high, x_band[...], preferred_element_type=jnp.float32)
                    + jnp.dot(low, x_band[...], preferred_element_type=jnp.float32))
        row = lax.broadcasted_iota(jnp.int32, (CHUNK, cols), 0) + (pencil * rows + r)
        col = lax.broadcasted_iota(jnp.int32, (CHUNK, cols), 1)
        cover_y = coverage(row, rows * pencils)
        cover_x = coverage(col, cols)
        for layer in range(depth):
            depth_index = jnp.full((1, cols), slab * depth + layer, jnp.int32)
            cover = coverage(depth_index, slabs * depth) * cover_y * cover_x
            filtered = smoothed[layer * CHUNK : (layer + 1) * CHUNK] / cover
            which = kinds[layer, pl.ds(r, CHUNK), :]
            value = jnp.where(which == 0, filtered, jnp.where(which == 2, FAR, -FAR))
            coded[layer, pl.ds(r, CHUNK), :] = value
            tangent = jnp.tanh(beta * (value - 0.5))
            acc[0] += folded(tangent)
            acc[1] += folded(1.0 - tangent * tangent)

    @pl.loop(0, steps + 1)
    def _(k):
        @pl.when(k < steps)
        def _():
            @pl.when(k + WINDOW < steps)
            def _():
                send_chunk(k + WINDOW)

            @pl.when(has_below)
            def _():
                up_copy(k).wait_recv()

                @pl.when(k == 0)
                def _():
                    below_halo.start()

            @pl.when(has_above)
            def _():
                down_copy(k).wait_recv()

                @pl.when(k == 0)
                def _():
                    above_halo.start()

            @pl.when(k == 0)
            def _():
                own_load.wait()
                kind_load.wait()

            filter_z(row_of(k) + PAD, CHUNK)

        @pl.when(k == 1)
        def _():
            own_halo.wait_recv()

            @pl.when(has_below)
            def _():
                below_halo.wait_recv()

            @pl.when(has_above)
            def _():
                above_halo.wait_recv()

            filter_z(halo, PAD)

        @pl.when(k >= 1)
        def _():
            filter_yx(k - 1)

    cells = float(devices) * float(depth * rows * cols)
    level = jnp.full((1, 1), 0.5, jnp.float32)
    for step in range(ITERS):
        if step:
            center = jnp.broadcast_to(level, (8, cols))

            def body(i, carry):
                total, bend = carry
                for layer in range(depth):
                    tangent = jnp.tanh(beta * (coded[layer, pl.ds(pl.multiple_of(i * 8, 8), 8), :] - center))
                    total = total + tangent
                    bend = bend + (1.0 - tangent * tangent)
                return total, bend

            zero = jnp.zeros((8, cols), jnp.float32)
            total, bend = lax.fori_loop(0, rows // 8, body, (zero, zero), unroll=2)
            total, bend = folded(total), folded(bend)
        else:
            total, bend = acc[0], acc[1]
        parts[step, me] = jnp.concatenate(
            [jnp.sum(total, axis=0, keepdims=True), jnp.sum(bend, axis=0, keepdims=True)], axis=0)

        def send(there, core):
            pltpu.make_async_remote_copy(
                parts.at[step, me], parts.at[step, me], r_send.at[step], r_recv.at[step],
                device_id=(there, core), device_id_type=MESH).start()

        def send_all(k, carry):
            there = slab + (slabs - k)
            there = there - jnp.where(there >= slabs, slabs, 0)
            for core in range(pencils):
                send(there, core)
            return carry

        lax.fori_loop(1, slabs, send_all, 0, unroll=15 if slabs % 15 == 1 else 1)
        send(slab, sibling)

        most = parts.at[step, pl.ds(0, devices - 1)]
        pltpu.make_async_copy(most, most, r_recv.at[step]).wait()
        both = jnp.sum(jnp.sum(parts[step], axis=0), axis=1, keepdims=True)
        volume = 0.5 * (cells + both[0:1])
        slope = cells + 0.5 * beta * both[1:2]
        level = level + (volume - fraction_ref[0] * cells) / slope
    level_out[...] = jnp.broadcast_to(level, level_out.shape)

    @pl.loop(0, steps)
    def _(k):
        @pl.when(has_above)
        def _():
            up_copy(k).wait_send()

        @pl.when(has_below)
        def _():
            down_copy(k).wait_send()

    own_halo.wait_send()

    @pl.when(has_below)
    def _():
        below_halo.wait_send()

    @pl.when(has_above)
    def _():
        above_halo.wait_send()

    for step in range(ITERS):
        most = parts.at[step, pl.ds(0, devices - 1)]
        pltpu.make_async_copy(most, most, r_send.at[step]).wait()


def solution(mesh):
    slabs, pencils = mesh.shape["slab"], mesh.shape["pencil"]

    def local(density, cell_kind, sharpness, fraction):
        depth, rows, cols = density.shape
        steps = rows // CHUNK
        wide = rows + 2 * PAD
        coded, level = pl.pallas_call(
            functools.partial(kernel, slabs, pencils),
            out_shape=(jax.ShapeDtypeStruct(density.shape, jnp.float32), jax.ShapeDtypeStruct((1, LANES), jnp.float32)),
            in_specs=[pl.BlockSpec(memory_space=pltpu.SMEM)] * 2 + [pl.BlockSpec(memory_space=pltpu.HBM)] * 2,
            out_specs=(pl.BlockSpec(memory_space=pltpu.VMEM), pl.BlockSpec(memory_space=pltpu.VMEM)),
            scratch_shapes=[
                pltpu.VMEM((depth, wide, cols), jnp.float32),
                pltpu.VMEM((RADIUS, wide, cols), jnp.float32),
                pltpu.VMEM((RADIUS, wide, cols), jnp.float32),
                pltpu.VMEM((depth, rows, cols), jnp.int32),
                pltpu.VMEM((depth, wide, cols), jnp.float32),
                pltpu.VMEM((cols, cols), jnp.bfloat16),
                pltpu.VMEM((2, 8, LANES), jnp.float32),
                pltpu.VMEM((ITERS, slabs * pencils, 2, LANES), jnp.float32),
                pltpu.SemaphoreType.DMA((steps,)),
                pltpu.SemaphoreType.DMA((steps,)),
                pltpu.SemaphoreType.DMA((steps,)),
                pltpu.SemaphoreType.DMA((steps,)),
                pltpu.SemaphoreType.DMA((3,)),
                pltpu.SemaphoreType.DMA((3,)),
                pltpu.SemaphoreType.DMA((2,)),
                pltpu.SemaphoreType.DMA((ITERS,)),
                pltpu.SemaphoreType.DMA((ITERS,)),
            ],
            compiler_params=pltpu.CompilerParams(
                collective_id=0, has_side_effects=True, vmem_limit_bytes=49 * 1024 * 1024),
        )(sharpness, fraction, density, cell_kind)
        threshold = level[0, :1]
        physical = 0.5 * (1.0 + jnp.tanh(sharpness[0] * (coded - threshold[0])))
        return physical, threshold

    in_specs = (P("slab", "pencil", None), P("slab", "pencil", None), P(), P())
    out_specs = (P("slab", "pencil", None), P())
    return jax.shard_map(local, mesh=mesh, in_specs=in_specs, out_specs=out_specs, check_vma=False)
```

```python
import functools
import itertools
import math

import jax
import jax.numpy as jnp
from jax import lax
from jax.experimental import pallas as pl
from jax.experimental.pallas import tpu as pltpu
from jax.sharding import PartitionSpec as P

RADIUS = 5
ITERS = 3
CHUNK = 16
PAD = 8
LANES = 128
HALF = 64
WAIT = 5
GRID = (4, 8, 4)
FAR = 1.0e6
MESH = pl.DeviceIdType.MESH


def box(values):
    pairs = [a + b for a, b in zip(values[:-1], values[1:])]
    return [pairs[k] + pairs[k + 2] + pairs[k + 4] for k in range(len(values) - RADIUS)]


def triangle(k):
    k = jnp.maximum(k, 0)
    return (k * (k + 1)) // 2


def coverage(index, whole):
    full = (RADIUS + 1) * (RADIUS + 1)
    return (full - triangle(RADIUS - index) - triangle(RADIUS + 1 + index - whole)).astype(jnp.float32)


def split(x):
    high = x.astype(jnp.bfloat16)
    return high, (x - high.astype(jnp.float32)).astype(jnp.bfloat16)


def band(shape, shift):
    row = lax.broadcasted_iota(jnp.int32, shape, 0)
    col = lax.broadcasted_iota(jnp.int32, shape, 1)
    return jnp.maximum(RADIUS + 1 - jnp.abs(col - shift - row), 0).astype(jnp.float32).astype(jnp.bfloat16)


def folded(x):
    tiles = [
        x[i : i + 8, j : j + LANES] for i in range(0, x.shape[0], 8) for j in range(0, x.shape[1], LANES)
    ]
    while len(tiles) > 1:
        tiles = [sum(tiles[i : i + 2][1:], tiles[i]) for i in range(0, len(tiles), 2)]
    return tiles[0]


def distance(offset, sizes):
    return sum(min(o, n - o) for o, n in zip(offset, sizes))


def kernel(slabs, pencils, grid, beta_in, fraction_in, density, kind, coded, level_out, own, below, above, kinds,
           along_z, x_band, acc, pair, parts, beta_ref, fraction_ref, u_send, u_recv, d_send, d_recv, h_send, h_recv,
           local_sem, p_send, p_recv, r_send, r_recv, known):
    depth, rows, cols = density.shape
    steps = rows // CHUNK
    reach = max((slabs - 1).bit_length() - 1, 1)
    slab = lax.axis_index("slab")
    pencil = lax.axis_index("pencil")
    first = pencil == 0
    devices = slabs * pencils

    barrier = pltpu.get_barrier_semaphore()

    def around(step):
        there = slab + (step if step > 0 else slabs + step)
        return there - jnp.where(there >= slabs, slabs, 0)

    for step in (1, -1):
        pl.semaphore_signal(barrier, inc=1, device_id=(around(step), pencil), device_id_type=MESH)
    pl.semaphore_signal(barrier, inc=1, device_id=(slab, 1 - pencil), device_id_type=MESH)

    def spread(j):
        for step in (1 << j, -(1 << j)):
            pl.semaphore_signal(known.at[j], inc=1, device_id=(around(step), pencil), device_id_type=MESH)

    has_above = slab + 1 < slabs
    has_below = slab > 0
    upper = jnp.minimum(slab + 1, slabs - 1)
    lower = jnp.maximum(slab - 1, 0)
    sibling = 1 - pencil
    halo = pl.multiple_of(jnp.where(first, PAD + rows, 0), 8)
    edge = pl.multiple_of(jnp.where(first, 0, PAD + rows), 8)
    there = pl.multiple_of(jnp.where(first, 0, PAD + rows), 8)
    mine = pl.multiple_of(jnp.where(first, rows, PAD), 8)

    def row_of(k):
        return pl.multiple_of(jnp.where(first, steps - 1 - k, k) * CHUNK, CHUNK)

    def up_copy(k):
        r = row_of(k)
        return pltpu.make_async_remote_copy(
            density.at[pl.ds(depth - RADIUS, RADIUS), pl.ds(r, CHUNK), :], below.at[:, pl.ds(r + PAD, CHUNK), :],
            u_send.at[k], u_recv.at[k], device_id=(upper, pencil), device_id_type=MESH)

    def down_copy(k):
        r = row_of(k)
        return pltpu.make_async_remote_copy(
            density.at[pl.ds(0, RADIUS), pl.ds(r, CHUNK), :], above.at[:, pl.ds(r + PAD, CHUNK), :],
            d_send.at[k], d_recv.at[k], device_id=(lower, pencil), device_id_type=MESH)

    def halo_copy(index, src, dst):
        return pltpu.make_async_remote_copy(
            src, dst, h_send.at[index], h_recv.at[index], device_id=(slab, sibling), device_id_type=MESH)

    own_row = pl.multiple_of(jnp.where(first, rows - PAD, 0), 8)
    own_halo = halo_copy(0, density.at[:, pl.ds(own_row, PAD), :], own.at[:, pl.ds(there, PAD), :])
    below_halo = halo_copy(1, below.at[:, pl.ds(mine, PAD), :], below.at[:, pl.ds(there, PAD), :])
    above_halo = halo_copy(2, above.at[:, pl.ds(mine, PAD), :], above.at[:, pl.ds(there, PAD), :])
    own_load = pltpu.make_async_copy(density, own.at[:, pl.ds(PAD, rows), :], local_sem.at[0])
    kind_load = pltpu.make_async_copy(kind, kinds, local_sem.at[1])
    beta_load = pltpu.make_async_copy(beta_in, beta_ref, local_sem.at[2])
    fraction_load = pltpu.make_async_copy(fraction_in, fraction_ref, local_sem.at[3])

    own_load.start()
    kind_load.start()
    beta_load.start()
    fraction_load.start()
    pl.semaphore_wait(barrier, 3)

    def send_chunk(k):
        @pl.when(has_above)
        def _():
            up_copy(k).start()

        @pl.when(has_below)
        def _():
            down_copy(k).start()

    send_chunk(0)
    own_halo.start()
    pl.loop(1, steps)(send_chunk)
    spread(0)

    x_band[...] = band((cols, cols), 0)
    acc[...] = jnp.zeros_like(acc)
    along_z[:, pl.ds(edge, PAD), :] = jnp.zeros((depth, PAD, cols), jnp.float32)

    @pl.when(jnp.logical_not(has_below))
    def _():
        @pl.loop(0, RADIUS)
        def _(k):
            below[k] = jnp.zeros(below.shape[1:], jnp.float32)

    @pl.when(jnp.logical_not(has_above))
    def _():
        @pl.loop(0, RADIUS)
        def _(k):
            above[k] = jnp.zeros(above.shape[1:], jnp.float32)

    beta_load.wait()
    fraction_load.wait()
    beta = beta_ref[0]

    def filter_z(start, count):
        for r in range(0, count, 8):
            for c in range(0, cols, LANES):
                at = (pl.ds(pl.multiple_of(start + r, 8), 8), pl.ds(c, LANES))
                values = [below[m, at[0], at[1]] for m in range(RADIUS)]
                values += [own[i, at[0], at[1]] for i in range(depth)]
                values += [above[i, at[0], at[1]] for i in range(RADIUS)]
                for i, out in enumerate(box(box(values))):
                    along_z[i, at[0], at[1]] = out

    def filter_yx(j):
        r = row_of(j)
        y_band = band((CHUNK, CHUNK + 2 * PAD), PAD)
        pieces = []
        for layer in range(depth):
            high, low = split(along_z[layer, pl.ds(r, CHUNK + 2 * PAD), :])
            pieces.append(jnp.dot(y_band, high, preferred_element_type=jnp.float32)
                          + jnp.dot(y_band, low, preferred_element_type=jnp.float32))
        high, low = split(jnp.concatenate(pieces, axis=0))
        smoothed = (jnp.dot(high, x_band[...], preferred_element_type=jnp.float32)
                    + jnp.dot(low, x_band[...], preferred_element_type=jnp.float32))
        row = lax.broadcasted_iota(jnp.int32, (CHUNK, cols), 0) + (pencil * rows + r)
        col = lax.broadcasted_iota(jnp.int32, (CHUNK, cols), 1)
        cover_y = coverage(row, rows * pencils)
        cover_x = coverage(col, cols)
        for layer in range(depth):
            depth_index = jnp.full((1, cols), slab * depth + layer, jnp.int32)
            cover = coverage(depth_index, slabs * depth) * cover_y * cover_x
            filtered = smoothed[layer * CHUNK : (layer + 1) * CHUNK] / cover
            which = kinds[layer, pl.ds(r, CHUNK), :]
            value = jnp.where(which == 0, beta * filtered, jnp.where(which == 2, FAR, -FAR))
            coded[layer, pl.ds(r, CHUNK), :] = value
            tangent = jnp.tanh(value - 0.5 * beta)
            acc[0] += folded(tangent)
            acc[1] += folded(1.0 - tangent * tangent)

    @pl.loop(0, steps + 1)
    def _(k):
        @pl.when(k < steps)
        def _():
            @pl.when(has_below)
            def _():
                up_copy(k).wait_recv()

                @pl.when(k == 0)
                def _():
                    below_halo.start()

            @pl.when(has_above)
            def _():
                down_copy(k).wait_recv()

                @pl.when(k == 0)
                def _():
                    above_halo.start()

            @pl.when(k == 0)
            def _():
                own_load.wait()
                kind_load.wait()

            filter_z(row_of(k) + PAD, CHUNK)

        @pl.when(k == 1)
        def _():
            own_halo.wait_recv()

            @pl.when(has_below)
            def _():
                below_halo.wait_recv()

            @pl.when(has_above)
            def _():
                above_halo.wait_recv()

            filter_z(halo, PAD)

        @pl.when(k >= 1)
        def _():
            filter_yx(k - 1)

        for j in range(reach):
            @pl.when(k == WAIT + j)
            def _():
                pl.semaphore_wait(known.at[j], 2)
                if j + 1 < reach:
                    spread(j + 1)

    cells = float(devices) * float(depth * rows * cols)
    offsets = [o for o in itertools.product(*(range(n) for n in grid)) if any(o)]
    offsets.sort(key=lambda o: -distance(o, grid))
    far_half = offsets[: slabs // 2]
    near_half = offsets[slabs // 2 :]
    lane = lax.broadcasted_iota(jnp.int32, (1, LANES), 1)

    def shifted(offset):
        there, place, scale = 0, slab, slabs
        for o, n in zip(offset, grid):
            scale //= n
            at = place // scale
            place = place - at * scale
            at = at + o
            there = there + jnp.where(at >= n, at - n, at) * scale
        return there

    level = jnp.full((1, 1), 0.5, jnp.float32)
    for step in range(ITERS):
        if step:
            center = jnp.broadcast_to(beta * level, (8, cols))

            def body(i, carry):
                total, bend = carry
                for layer in range(depth):
                    tangent = jnp.tanh(coded[layer, pl.ds(pl.multiple_of(i * 8, 8), 8), :] - center)
                    total = total + tangent
                    bend = bend + (1.0 - tangent * tangent)
                return total, bend

            zero = jnp.zeros((8, cols), jnp.float32)
            total, bend = lax.fori_loop(0, rows // 8, body, (zero, zero), unroll=2)
            total, bend = folded(total), folded(bend)
        else:
            total, bend = acc[0], acc[1]
        total = jnp.sum(total, axis=0, keepdims=True)
        bend = jnp.sum(bend, axis=0, keepdims=True)
        total = total + pltpu.roll(total, HALF, 1)
        bend = bend + pltpu.roll(bend, HALF, 1)
        pair[step, 0] = jnp.where(lane < HALF, total, bend)
        swap = pltpu.make_async_remote_copy(
            pair.at[step, 0], pair.at[step, 1], p_send.at[step], p_recv.at[step],
            device_id=(slab, sibling), device_id_type=MESH)
        swap.start()
        swap.wait_recv()
        parts[step, slab] = pair[step, 0] + pair[step, 1]

        def send(there, core):
            pltpu.make_async_remote_copy(
                parts.at[step, slab], parts.at[step, slab], r_send.at[step], r_recv.at[step],
                device_id=(there, core), device_id_type=MESH).start()

        for here, chips in ((pencils - 1, far_half), (0, near_half)):
            @pl.when(pencil == here)
            def _():
                for offset in chips:
                    there = shifted(offset)
                    for core in range(pencils):
                        send(there, core)

        most = parts.at[step, pl.ds(0, slabs - 1)]
        pltpu.make_async_copy(most, most, r_recv.at[step]).wait()
        both = jnp.sum(parts[step], axis=0)
        volume = 0.5 * (cells + jnp.sum(jnp.where(lane < HALF, both, 0.0), axis=1, keepdims=True))
        slope = cells + 0.5 * beta * jnp.sum(jnp.where(lane < HALF, 0.0, both), axis=1, keepdims=True)
        level = level + (volume - fraction_ref[0] * cells) / slope
    level_out[...] = jnp.broadcast_to(level, level_out.shape)

    @pl.loop(0, steps)
    def _(k):
        @pl.when(has_above)
        def _():
            up_copy(k).wait_send()

        @pl.when(has_below)
        def _():
            down_copy(k).wait_send()

    own_halo.wait_send()

    @pl.when(has_below)
    def _():
        below_halo.wait_send()

    @pl.when(has_above)
    def _():
        above_halo.wait_send()

    for step in range(ITERS):
        pltpu.make_async_copy(pair.at[step, 0], pair.at[step, 0], p_send.at[step]).wait()

    for here, chips in ((pencils - 1, far_half), (0, near_half)):
        @pl.when(pencil == here)
        def _():
            for step in range(ITERS):
                most = parts.at[step, pl.ds(0, len(chips))]
                for core in range(pencils):
                    pltpu.make_async_copy(most, most, r_send.at[step]).wait()


def solution(mesh):
    slabs, pencils = mesh.shape["slab"], mesh.shape["pencil"]
    grid = GRID if math.prod(GRID) == slabs else (slabs,)

    def local(density, cell_kind, sharpness, fraction):
        depth, rows, cols = density.shape
        steps = rows // CHUNK
        wide = rows + 2 * PAD
        coded, level = pl.pallas_call(
            functools.partial(kernel, slabs, pencils, grid),
            out_shape=(jax.ShapeDtypeStruct(density.shape, jnp.float32), jax.ShapeDtypeStruct((1, LANES), jnp.float32)),
            in_specs=[pl.BlockSpec(memory_space=pltpu.HBM)] * 4,
            out_specs=(pl.BlockSpec(memory_space=pltpu.VMEM), pl.BlockSpec(memory_space=pltpu.VMEM)),
            scratch_shapes=[
                pltpu.VMEM((depth, wide, cols), jnp.float32),
                pltpu.VMEM((RADIUS, wide, cols), jnp.float32),
                pltpu.VMEM((RADIUS, wide, cols), jnp.float32),
                pltpu.VMEM((depth, rows, cols), jnp.int32),
                pltpu.VMEM((depth, wide, cols), jnp.float32),
                pltpu.VMEM((cols, cols), jnp.bfloat16),
                pltpu.VMEM((2, 8, LANES), jnp.float32),
                pltpu.VMEM((ITERS, 2, 1, LANES), jnp.float32),
                pltpu.VMEM((ITERS, slabs, 1, LANES), jnp.float32),
                pltpu.SMEM((1,), jnp.float32),
                pltpu.SMEM((1,), jnp.float32),
                pltpu.SemaphoreType.DMA((steps,)),
                pltpu.SemaphoreType.DMA((steps,)),
                pltpu.SemaphoreType.DMA((steps,)),
                pltpu.SemaphoreType.DMA((steps,)),
                pltpu.SemaphoreType.DMA((3,)),
                pltpu.SemaphoreType.DMA((3,)),
                pltpu.SemaphoreType.DMA((4,)),
                pltpu.SemaphoreType.DMA((ITERS,)),
                pltpu.SemaphoreType.DMA((ITERS,)),
                pltpu.SemaphoreType.DMA((ITERS,)),
                pltpu.SemaphoreType.DMA((ITERS,)),
                pltpu.SemaphoreType.REGULAR((max((slabs - 1).bit_length() - 1, 1),)),
            ],
            compiler_params=pltpu.CompilerParams(
                collective_id=0, has_side_effects=True, vmem_limit_bytes=49 * 1024 * 1024),
        )(sharpness, fraction, density, cell_kind)
        threshold = level[0, :1]
        physical = 0.5 * (1.0 + jnp.tanh(coded - sharpness[0] * threshold[0]))
        return physical, threshold

    in_specs = (P("slab", "pencil", None), P("slab", "pencil", None), P(), P())
    out_specs = (P("slab", "pencil", None), P())
    return jax.shard_map(local, mesh=mesh, in_specs=in_specs, out_specs=out_specs, check_vma=False)
```

```python
import functools
import itertools
import math

import jax
import jax.numpy as jnp
from jax import lax
from jax.experimental import pallas as pl
from jax.experimental.pallas import tpu as pltpu
from jax.sharding import PartitionSpec as P

RADIUS = 5
ITERS = 3
CHUNK = 16
PAD = 8
LANES = 128
HALF = 64
WAIT = 5
GRID = (4, 8, 4)
FAR = 1.0e6
MESH = pl.DeviceIdType.MESH


def box(values):
    pairs = [a + b for a, b in zip(values[:-1], values[1:])]
    return [pairs[k] + pairs[k + 2] + pairs[k + 4] for k in range(len(values) - RADIUS)]


def triangle(k):
    k = jnp.maximum(k, 0)
    return (k * (k + 1)) // 2


def coverage(index, whole):
    full = (RADIUS + 1) * (RADIUS + 1)
    return (full - triangle(RADIUS - index) - triangle(RADIUS + 1 + index - whole)).astype(jnp.float32)


def split(x):
    high = x.astype(jnp.bfloat16)
    return high, (x - high.astype(jnp.float32)).astype(jnp.bfloat16)


def band(shape, shift):
    row = lax.broadcasted_iota(jnp.int32, shape, 0)
    col = lax.broadcasted_iota(jnp.int32, shape, 1)
    return jnp.maximum(RADIUS + 1 - jnp.abs(col - shift - row), 0).astype(jnp.float32).astype(jnp.bfloat16)


def tree(parts):
    parts = list(parts)
    while len(parts) > 1:
        parts = [sum(parts[i : i + 2][1:], parts[i]) for i in range(0, len(parts), 2)]
    return parts[0]


def folded(x):
    return tree(x[i : i + 8, j : j + LANES] for i in range(0, x.shape[0], 8) for j in range(0, x.shape[1], LANES))


def distance(offset, sizes):
    return sum(min(o, n - o) for o, n in zip(offset, sizes))


def kernel(slabs, pencils, grid, beta_in, fraction_in, density, kind, coded, level_out, own, below, above, kinds,
           along_z, x_band, acc, pair, parts, beta_ref, fraction_ref, u_send, u_recv, d_send, d_recv, h_send, h_recv,
           local_sem, p_send, p_recv, r_send, r_recv, known):
    depth, rows, cols = density.shape
    steps = rows // CHUNK
    reach = max((slabs - 1).bit_length() - 1, 1)
    slab = lax.axis_index("slab")
    pencil = lax.axis_index("pencil")
    first = pencil == 0
    devices = slabs * pencils

    barrier = pltpu.get_barrier_semaphore()

    def around(step):
        there = slab + (step if step > 0 else slabs + step)
        return there - jnp.where(there >= slabs, slabs, 0)

    for step in (1, -1):
        pl.semaphore_signal(barrier, inc=1, device_id=(around(step), pencil), device_id_type=MESH)
    pl.semaphore_signal(barrier, inc=1, device_id=(slab, 1 - pencil), device_id_type=MESH)

    def spread(j):
        for step in (1 << j, -(1 << j)):
            pl.semaphore_signal(known.at[j], inc=1, device_id=(around(step), pencil), device_id_type=MESH)

    has_above = slab + 1 < slabs
    has_below = slab > 0
    upper = jnp.minimum(slab + 1, slabs - 1)
    lower = jnp.maximum(slab - 1, 0)
    sibling = 1 - pencil
    halo = pl.multiple_of(jnp.where(first, PAD + rows, 0), 8)
    edge = pl.multiple_of(jnp.where(first, 0, PAD + rows), 8)
    there = pl.multiple_of(jnp.where(first, 0, PAD + rows), 8)
    mine = pl.multiple_of(jnp.where(first, rows, PAD), 8)

    def row_of(k):
        return pl.multiple_of(jnp.where(first, steps - 1 - k, k) * CHUNK, CHUNK)

    def up_copy(k):
        r = row_of(k)
        return pltpu.make_async_remote_copy(
            density.at[pl.ds(depth - RADIUS, RADIUS), pl.ds(r, CHUNK), :], below.at[:, pl.ds(r + PAD, CHUNK), :],
            u_send.at[k], u_recv.at[k], device_id=(upper, pencil), device_id_type=MESH)

    def down_copy(k):
        r = row_of(k)
        return pltpu.make_async_remote_copy(
            density.at[pl.ds(0, RADIUS), pl.ds(r, CHUNK), :], above.at[:, pl.ds(r + PAD, CHUNK), :],
            d_send.at[k], d_recv.at[k], device_id=(lower, pencil), device_id_type=MESH)

    def halo_copy(index, src, dst):
        return pltpu.make_async_remote_copy(
            src, dst, h_send.at[index], h_recv.at[index], device_id=(slab, sibling), device_id_type=MESH)

    own_row = pl.multiple_of(jnp.where(first, rows - PAD, 0), 8)
    own_halo = halo_copy(0, density.at[:, pl.ds(own_row, PAD), :], own.at[:, pl.ds(there, PAD), :])
    below_halo = halo_copy(1, below.at[:, pl.ds(mine, PAD), :], below.at[:, pl.ds(there, PAD), :])
    above_halo = halo_copy(2, above.at[:, pl.ds(mine, PAD), :], above.at[:, pl.ds(there, PAD), :])
    own_load = pltpu.make_async_copy(density, own.at[:, pl.ds(PAD, rows), :], local_sem.at[0])
    kind_load = pltpu.make_async_copy(kind, kinds, local_sem.at[1])
    beta_load = pltpu.make_async_copy(beta_in, beta_ref, local_sem.at[2])
    fraction_load = pltpu.make_async_copy(fraction_in, fraction_ref, local_sem.at[3])

    own_load.start()
    kind_load.start()
    beta_load.start()
    fraction_load.start()
    pl.semaphore_wait(barrier, 3)

    def send_chunk(k):
        @pl.when(has_above)
        def _():
            up_copy(k).start()

        @pl.when(has_below)
        def _():
            down_copy(k).start()

    send_chunk(0)
    own_halo.start()
    pl.loop(1, steps)(send_chunk)
    spread(0)

    x_band[...] = band((cols, cols), 0)
    acc[...] = jnp.zeros_like(acc)
    along_z[:, pl.ds(edge, PAD), :] = jnp.zeros((depth, PAD, cols), jnp.float32)

    @pl.when(jnp.logical_not(has_below))
    def _():
        @pl.loop(0, RADIUS)
        def _(k):
            below[k] = jnp.zeros(below.shape[1:], jnp.float32)

    @pl.when(jnp.logical_not(has_above))
    def _():
        @pl.loop(0, RADIUS)
        def _(k):
            above[k] = jnp.zeros(above.shape[1:], jnp.float32)

    beta_load.wait()
    fraction_load.wait()
    beta = beta_ref[0]

    def filter_z(start, count):
        for r in range(0, count, 8):
            for c in range(0, cols, LANES):
                at = (pl.ds(pl.multiple_of(start + r, 8), 8), pl.ds(c, LANES))
                values = [below[m, at[0], at[1]] for m in range(RADIUS)]
                values += [own[i, at[0], at[1]] for i in range(depth)]
                values += [above[i, at[0], at[1]] for i in range(RADIUS)]
                for i, out in enumerate(box(box(values))):
                    along_z[i, at[0], at[1]] = out

    def filter_yx(j):
        r = row_of(j)
        y_band = band((CHUNK, CHUNK + 2 * PAD), PAD)
        pieces = []
        for layer in range(depth):
            high, low = split(along_z[layer, pl.ds(r, CHUNK + 2 * PAD), :])
            pieces.append(jnp.dot(y_band, high, preferred_element_type=jnp.float32)
                          + jnp.dot(y_band, low, preferred_element_type=jnp.float32))
        high, low = split(jnp.concatenate(pieces, axis=0))
        smoothed = (jnp.dot(high, x_band[...], preferred_element_type=jnp.float32)
                    + jnp.dot(low, x_band[...], preferred_element_type=jnp.float32))
        row = lax.broadcasted_iota(jnp.int32, (CHUNK, cols), 0) + (pencil * rows + r)
        col = lax.broadcasted_iota(jnp.int32, (CHUNK, cols), 1)
        cover_y = coverage(row, rows * pencils)
        cover_x = coverage(col, cols)
        for layer in range(depth):
            depth_index = jnp.full((1, cols), slab * depth + layer, jnp.int32)
            cover = coverage(depth_index, slabs * depth) * cover_y * cover_x
            filtered = smoothed[layer * CHUNK : (layer + 1) * CHUNK] / cover
            which = kinds[layer, pl.ds(r, CHUNK), :]
            value = jnp.where(which == 0, beta * filtered, jnp.where(which == 2, FAR, -FAR))
            coded[layer, pl.ds(r, CHUNK), :] = value
            tangent = jnp.tanh(value - 0.5 * beta)
            acc[0] += folded(tangent)
            acc[1] += folded(1.0 - tangent * tangent)

    @pl.loop(0, steps + 1)
    def _(k):
        @pl.when(k < steps)
        def _():
            @pl.when(has_below)
            def _():
                up_copy(k).wait_recv()

                @pl.when(k == 0)
                def _():
                    below_halo.start()

            @pl.when(has_above)
            def _():
                down_copy(k).wait_recv()

                @pl.when(k == 0)
                def _():
                    above_halo.start()

            @pl.when(k == 0)
            def _():
                own_load.wait()
                kind_load.wait()

            filter_z(row_of(k) + PAD, CHUNK)

        @pl.when(k == 1)
        def _():
            own_halo.wait_recv()

            @pl.when(has_below)
            def _():
                below_halo.wait_recv()

            @pl.when(has_above)
            def _():
                above_halo.wait_recv()

            filter_z(halo, PAD)

        @pl.when(k >= 1)
        def _():
            filter_yx(k - 1)

        for j in range(reach):
            @pl.when(k == WAIT + j)
            def _():
                pl.semaphore_wait(known.at[j], 2)
                if j + 1 < reach:
                    spread(j + 1)

    cells = float(devices) * float(depth * rows * cols)
    offsets = [o for o in itertools.product(*(range(n) for n in grid)) if any(o)]
    offsets.sort(key=lambda o: -distance(o, grid))
    direct = [o for o in offsets if distance(o, grid) >= sum(n // 2 for n in grid) - 1]
    rest = offsets[len(direct) :]
    far_half = rest[: (len(rest) + 1) // 2]
    near_half = rest[(len(rest) + 1) // 2 :]
    arrivals = slabs - 1 + len(direct)
    lane = lax.broadcasted_iota(jnp.int32, (1, LANES), 1)

    def shifted(offset):
        there, place, scale = 0, slab, slabs
        for o, n in zip(offset, grid):
            scale //= n
            at = place // scale
            place = place - at * scale
            at = at + o
            there = there + jnp.where(at >= n, at - n, jnp.where(at < 0, at + n, at)) * scale
        return there

    def send(step, source, slot, there, core):
        pltpu.make_async_remote_copy(
            source, parts.at[step, slot], r_send.at[step], r_recv.at[step],
            device_id=(there, core), device_id_type=MESH).start()

    def newton(step, level):
        @pl.when(step > 0)
        def _():
            center = jnp.broadcast_to(beta * level, (8, LANES))

            def body(i, carry):
                total, bend = carry
                at = pl.ds(pl.multiple_of(i * 8, 8), 8)
                for layer in range(depth):
                    tangents = [jnp.tanh(coded[layer, at, pl.ds(c * LANES, LANES)] - center) for c in range(cols // LANES)]
                    total = tuple(a + t for a, t in zip(total, tangents))
                    bend = tuple(a + (1.0 - t * t) for a, t in zip(bend, tangents))
                return total, bend

            zero = (jnp.zeros((8, LANES), jnp.float32),) * (cols // LANES)
            total, bend = lax.fori_loop(0, rows // 8, body, (zero, zero), unroll=6)
            acc[0] = tree(total)
            acc[1] = tree(bend)

        total = jnp.sum(acc[0], axis=0, keepdims=True)
        bend = jnp.sum(acc[1], axis=0, keepdims=True)
        total = total + pltpu.roll(total, HALF, 1)
        bend = bend + pltpu.roll(bend, HALF, 1)
        pair[step, 0] = jnp.where(lane < HALF, total, bend)
        swap = pltpu.make_async_remote_copy(
            pair.at[step, 0], pair.at[step, 1], p_send.at[step], p_recv.at[step],
            device_id=(slab, sibling), device_id_type=MESH)
        swap.start()
        for j, offset in enumerate(direct):
            there = shifted(offset)
            for core in range(pencils):
                send(step, pair.at[step, 0], jnp.where(first, slab, slabs + j), there, core)
        swap.wait_recv()
        parts[step, slab] = pair[step, 0] + pair[step, 1]

        for here, chips in ((pencils - 1, far_half), (0, near_half)):
            @pl.when(pencil == here)
            def _():
                for offset in chips:
                    there = shifted(offset)
                    for core in range(pencils):
                        send(step, parts.at[step, slab], slab, there, core)

        most = parts.at[step, pl.ds(0, arrivals)]
        pltpu.make_async_copy(most, most, r_recv.at[step]).wait()
        for j, offset in enumerate(direct):
            there = shifted([-o for o in offset])
            parts[step, there] = parts[step, there] + parts[step, slabs + j]
        both = tree([parts[step, i] for i in range(slabs)])
        volume = 0.5 * (cells + jnp.sum(jnp.where(lane < HALF, both, 0.0), axis=1, keepdims=True))
        slope = cells + 0.5 * beta * jnp.sum(jnp.where(lane < HALF, 0.0, both), axis=1, keepdims=True)
        return level + (volume - fraction_ref[0] * cells) / slope

    level = lax.fori_loop(0, ITERS, newton, jnp.full((1, LANES), 0.5, jnp.float32))
    level_out[0:1] = level
    level_out[1:2] = beta * level

    @pl.loop(0, steps)
    def _(k):
        @pl.when(has_above)
        def _():
            up_copy(k).wait_send()

        @pl.when(has_below)
        def _():
            down_copy(k).wait_send()

    own_halo.wait_send()

    @pl.when(has_below)
    def _():
        below_halo.wait_send()

    @pl.when(has_above)
    def _():
        above_halo.wait_send()

    for step in range(ITERS):
        pltpu.make_async_copy(pair.at[step, 0], pair.at[step, 0], p_send.at[step]).wait()

    for here, chips in ((pencils - 1, far_half), (0, near_half)):
        @pl.when(pencil == here)
        def _():
            for step in range(ITERS):
                most = parts.at[step, pl.ds(0, len(direct) + len(chips))]
                for core in range(pencils):
                    pltpu.make_async_copy(most, most, r_send.at[step]).wait()


def project(coded, level, physical, threshold, held, level_held, sems, level_sem):
    depth, rows, cols = coded.shape
    center = jnp.broadcast_to(level[1:2], (8, LANES))
    level_held[0] = jnp.max(level[0:1])
    level_copy = pltpu.make_async_copy(level_held, threshold, level_sem)
    level_copy.start()
    copies = []
    for layer in range(depth):
        @pl.loop(0, rows // 8, unroll=16)
        def _(i):
            at = pl.ds(pl.multiple_of(i * 8, 8), 8)
            for c in range(0, cols, LANES):
                held[layer, at, pl.ds(c, LANES)] = 0.5 * (1.0 + jnp.tanh(coded[layer, at, pl.ds(c, LANES)] - center))

        copies.append(pltpu.make_async_copy(held.at[layer], physical.at[layer], sems.at[layer]))
        copies[-1].start()
    for copy in copies:
        copy.wait()
    level_copy.wait()


def solution(mesh):
    slabs, pencils = mesh.shape["slab"], mesh.shape["pencil"]
    grid = GRID if math.prod(GRID) == slabs else (slabs,)

    def local(density, cell_kind, sharpness, fraction):
        depth, rows, cols = density.shape
        steps = rows // CHUNK
        wide = rows + 2 * PAD
        coded, level = pl.pallas_call(
            functools.partial(kernel, slabs, pencils, grid),
            out_shape=(jax.ShapeDtypeStruct(density.shape, jnp.float32), jax.ShapeDtypeStruct((2, LANES), jnp.float32)),
            in_specs=[pl.BlockSpec(memory_space=pltpu.HBM)] * 4,
            out_specs=(pl.BlockSpec(memory_space=pltpu.VMEM), pl.BlockSpec(memory_space=pltpu.VMEM)),
            scratch_shapes=[
                pltpu.VMEM((depth, wide, cols), jnp.float32),
                pltpu.VMEM((RADIUS, wide, cols), jnp.float32),
                pltpu.VMEM((RADIUS, wide, cols), jnp.float32),
                pltpu.VMEM((depth, rows, cols), jnp.int32),
                pltpu.VMEM((depth, wide, cols), jnp.float32),
                pltpu.VMEM((cols, cols), jnp.bfloat16),
                pltpu.VMEM((2, 8, LANES), jnp.float32),
                pltpu.VMEM((ITERS, 2, 1, LANES), jnp.float32),
                pltpu.VMEM((ITERS, 2 * slabs, 1, LANES), jnp.float32),
                pltpu.SMEM((1,), jnp.float32),
                pltpu.SMEM((1,), jnp.float32),
                pltpu.SemaphoreType.DMA((steps,)),
                pltpu.SemaphoreType.DMA((steps,)),
                pltpu.SemaphoreType.DMA((steps,)),
                pltpu.SemaphoreType.DMA((steps,)),
                pltpu.SemaphoreType.DMA((3,)),
                pltpu.SemaphoreType.DMA((3,)),
                pltpu.SemaphoreType.DMA((4,)),
                pltpu.SemaphoreType.DMA((ITERS,)),
                pltpu.SemaphoreType.DMA((ITERS,)),
                pltpu.SemaphoreType.DMA((ITERS,)),
                pltpu.SemaphoreType.DMA((ITERS,)),
                pltpu.SemaphoreType.REGULAR((max((slabs - 1).bit_length() - 1, 1),)),
            ],
            compiler_params=pltpu.CompilerParams(
                collective_id=0, has_side_effects=True, vmem_limit_bytes=49 * 1024 * 1024),
        )(sharpness, fraction, density, cell_kind)
        return pl.pallas_call(
            project,
            out_shape=(jax.ShapeDtypeStruct(density.shape, jnp.float32), jax.ShapeDtypeStruct((1,), jnp.float32)),
            in_specs=[pl.BlockSpec(memory_space=pltpu.VMEM)] * 2,
            out_specs=(pl.BlockSpec(memory_space=pltpu.HBM), pl.BlockSpec(memory_space=pltpu.HBM)),
            scratch_shapes=[
                pltpu.VMEM(density.shape, jnp.float32),
                pltpu.SMEM((1,), jnp.float32),
                pltpu.SemaphoreType.DMA((depth,)),
                pltpu.SemaphoreType.DMA,
            ],
            compiler_params=pltpu.CompilerParams(vmem_limit_bytes=8 * 1024 * 1024),
        )(coded, level)

    in_specs = (P("slab", "pencil", None), P("slab", "pencil", None), P(), P())
    out_specs = (P("slab", "pencil", None), P())
    return jax.shard_map(local, mesh=mesh, in_specs=in_specs, out_specs=out_specs, check_vma=False)
```

```python
import functools
import itertools
import math

import jax
import jax.numpy as jnp
from jax import lax
from jax.experimental import pallas as pl
from jax.experimental.pallas import tpu as pltpu
from jax.sharding import PartitionSpec as P

RADIUS = 5
ITERS = 3
CHUNK = 16
PAD = 8
LANES = 128
HALF = 64
NEARER = 2
WAIT = 5
GRID = (4, 8, 4)
FAR = 1.0e6
MESH = pl.DeviceIdType.MESH


def box(values):
    pairs = [a + b for a, b in zip(values[:-1], values[1:])]
    return [pairs[k] + pairs[k + 2] + pairs[k + 4] for k in range(len(values) - RADIUS)]


def triangle(k):
    k = jnp.maximum(k, 0)
    return (k * (k + 1)) // 2


def coverage(index, whole):
    full = (RADIUS + 1) * (RADIUS + 1)
    return (full - triangle(RADIUS - index) - triangle(RADIUS + 1 + index - whole)).astype(jnp.float32)


def split(x):
    high = x.astype(jnp.bfloat16)
    return high, (x - high.astype(jnp.float32)).astype(jnp.bfloat16)


def band(shape, shift):
    row = lax.broadcasted_iota(jnp.int32, shape, 0)
    col = lax.broadcasted_iota(jnp.int32, shape, 1)
    return jnp.maximum(RADIUS + 1 - jnp.abs(col - shift - row), 0).astype(jnp.float32).astype(jnp.bfloat16)


def tree(parts):
    parts = list(parts)
    while len(parts) > 1:
        parts = [sum(parts[i : i + 2][1:], parts[i]) for i in range(0, len(parts), 2)]
    return parts[0]


def folded(x):
    return tree(x[i : i + 8, j : j + LANES] for i in range(0, x.shape[0], 8) for j in range(0, x.shape[1], LANES))


def distance(offset, sizes):
    return sum(min(o, n - o) for o, n in zip(offset, sizes))


def kernel(slabs, pencils, grid, beta_in, fraction_in, density, kind, coded, level_out, own, below, above, kinds,
           along_z, x_band, acc, pair, parts, beta_ref, fraction_ref, u_send, u_recv, d_send, d_recv, h_send, h_recv,
           local_sem, p_send, p_recv, r_send, r_recv, known):
    depth, rows, cols = density.shape
    steps = rows // CHUNK
    reach = max((slabs - 1).bit_length() - 1, 1)
    slab = lax.axis_index("slab")
    pencil = lax.axis_index("pencil")
    first = pencil == 0
    devices = slabs * pencils

    barrier = pltpu.get_barrier_semaphore()

    def around(step):
        there = slab + (step if step > 0 else slabs + step)
        return there - jnp.where(there >= slabs, slabs, 0)

    for step in (1, -1):
        pl.semaphore_signal(barrier, inc=1, device_id=(around(step), pencil), device_id_type=MESH)
    pl.semaphore_signal(barrier, inc=1, device_id=(slab, 1 - pencil), device_id_type=MESH)

    def spread(j):
        for step in (1 << j, -(1 << j)):
            pl.semaphore_signal(known.at[j], inc=1, device_id=(around(step), pencil), device_id_type=MESH)

    has_above = slab + 1 < slabs
    has_below = slab > 0
    upper = jnp.minimum(slab + 1, slabs - 1)
    lower = jnp.maximum(slab - 1, 0)
    sibling = 1 - pencil
    halo = pl.multiple_of(jnp.where(first, PAD + rows, 0), 8)
    edge = pl.multiple_of(jnp.where(first, 0, PAD + rows), 8)
    there = pl.multiple_of(jnp.where(first, 0, PAD + rows), 8)
    mine = pl.multiple_of(jnp.where(first, rows, PAD), 8)

    def row_of(k):
        return pl.multiple_of(jnp.where(first, steps - 1 - k, k) * CHUNK, CHUNK)

    def up_copy(k):
        r = row_of(k)
        return pltpu.make_async_remote_copy(
            density.at[pl.ds(depth - RADIUS, RADIUS), pl.ds(r, CHUNK), :], below.at[:, pl.ds(r + PAD, CHUNK), :],
            u_send.at[k], u_recv.at[k], device_id=(upper, pencil), device_id_type=MESH)

    def down_copy(k):
        r = row_of(k)
        return pltpu.make_async_remote_copy(
            density.at[pl.ds(0, RADIUS), pl.ds(r, CHUNK), :], above.at[:, pl.ds(r + PAD, CHUNK), :],
            d_send.at[k], d_recv.at[k], device_id=(lower, pencil), device_id_type=MESH)

    def halo_copy(index, src, dst):
        return pltpu.make_async_remote_copy(
            src, dst, h_send.at[index], h_recv.at[index], device_id=(slab, sibling), device_id_type=MESH)

    own_row = pl.multiple_of(jnp.where(first, rows - PAD, 0), 8)
    own_halo = halo_copy(0, density.at[:, pl.ds(own_row, PAD), :], own.at[:, pl.ds(there, PAD), :])
    below_halo = halo_copy(1, below.at[:, pl.ds(mine, PAD), :], below.at[:, pl.ds(there, PAD), :])
    above_halo = halo_copy(2, above.at[:, pl.ds(mine, PAD), :], above.at[:, pl.ds(there, PAD), :])
    own_load = pltpu.make_async_copy(density, own.at[:, pl.ds(PAD, rows), :], local_sem.at[0])
    kind_load = pltpu.make_async_copy(kind, kinds, local_sem.at[1])
    beta_load = pltpu.make_async_copy(beta_in, beta_ref, local_sem.at[2])
    fraction_load = pltpu.make_async_copy(fraction_in, fraction_ref, local_sem.at[3])

    own_load.start()
    kind_load.start()
    beta_load.start()
    fraction_load.start()
    pl.semaphore_wait(barrier, 3)

    def send_chunk(k):
        @pl.when(has_above)
        def _():
            up_copy(k).start()

        @pl.when(has_below)
        def _():
            down_copy(k).start()

    pl.loop(0, steps)(send_chunk)
    parts[:, slabs:] = jnp.zeros((ITERS, slabs, 1, LANES), jnp.float32)
    own_halo.start()

    x_band[...] = band((cols, cols), 0)
    acc[...] = jnp.zeros_like(acc)
    along_z[:, pl.ds(edge, PAD), :] = jnp.zeros((depth, PAD, cols), jnp.float32)

    @pl.when(jnp.logical_not(has_below))
    def _():
        @pl.loop(0, RADIUS)
        def _(k):
            below[k] = jnp.zeros(below.shape[1:], jnp.float32)

    @pl.when(jnp.logical_not(has_above))
    def _():
        @pl.loop(0, RADIUS)
        def _(k):
            above[k] = jnp.zeros(above.shape[1:], jnp.float32)

    beta_load.wait()
    fraction_load.wait()
    beta = beta_ref[0]

    def filter_z(start, count):
        for r in range(0, count, 8):
            for c in range(0, cols, LANES):
                at = (pl.ds(pl.multiple_of(start + r, 8), 8), pl.ds(c, LANES))
                values = [below[m, at[0], at[1]] for m in range(RADIUS)]
                values += [own[i, at[0], at[1]] for i in range(depth)]
                values += [above[i, at[0], at[1]] for i in range(RADIUS)]
                for i, out in enumerate(box(box(values))):
                    along_z[i, at[0], at[1]] = out

    def filter_yx(j):
        r = row_of(j)
        y_band = band((CHUNK, CHUNK + 2 * PAD), PAD)
        pieces = []
        for layer in range(depth):
            high, low = split(along_z[layer, pl.ds(r, CHUNK + 2 * PAD), :])
            pieces.append(jnp.dot(y_band, high, preferred_element_type=jnp.float32)
                          + jnp.dot(y_band, low, preferred_element_type=jnp.float32))
        high, low = split(jnp.concatenate(pieces, axis=0))
        smoothed = (jnp.dot(high, x_band[...], preferred_element_type=jnp.float32)
                    + jnp.dot(low, x_band[...], preferred_element_type=jnp.float32))
        row = lax.broadcasted_iota(jnp.int32, (CHUNK, cols), 0) + (pencil * rows + r)
        col = lax.broadcasted_iota(jnp.int32, (CHUNK, cols), 1)
        cover_y = coverage(row, rows * pencils)
        cover_x = coverage(col, cols)
        for layer in range(depth):
            depth_index = jnp.full((1, cols), slab * depth + layer, jnp.int32)
            cover = coverage(depth_index, slabs * depth) * cover_y * cover_x
            filtered = smoothed[layer * CHUNK : (layer + 1) * CHUNK] / cover
            which = kinds[layer, pl.ds(r, CHUNK), :]
            value = jnp.where(which == 0, beta * filtered, jnp.where(which == 2, FAR, -FAR))
            coded[layer, pl.ds(r, CHUNK), :] = value
            tangent = jnp.tanh(value - 0.5 * beta)
            acc[0] += folded(tangent)
            acc[1] += folded(1.0 - tangent * tangent)

    @pl.loop(0, steps + 1)
    def _(k):
        @pl.when(k < steps)
        def _():
            @pl.when(has_below)
            def _():
                up_copy(k).wait_recv()

                @pl.when(k == 0)
                def _():
                    below_halo.start()

            @pl.when(has_above)
            def _():
                down_copy(k).wait_recv()

                @pl.when(k == 0)
                def _():
                    above_halo.start()

            @pl.when(k == 0)
            def _():
                own_load.wait()
                kind_load.wait()

            filter_z(row_of(k) + PAD, CHUNK)

        @pl.when(k == 1)
        def _():
            own_halo.wait_recv()

            @pl.when(has_below)
            def _():
                below_halo.wait_recv()

            @pl.when(has_above)
            def _():
                above_halo.wait_recv()

            filter_z(halo, PAD)

        @pl.when(k >= 1)
        def _():
            filter_yx(k - 1)

        @pl.when(k == WAIT - 1)
        def _():
            spread(0)

        for j in range(reach):
            @pl.when(k == WAIT + j)
            def _():
                pl.semaphore_wait(known.at[j], 2)
                if j + 1 < reach:
                    spread(j + 1)

    cells = float(devices) * float(depth * rows * cols)
    offsets = [o for o in itertools.product(*(range(n) for n in grid)) if any(o)]
    offsets.sort(key=lambda o: -distance(o, grid))
    direct = [o for o in offsets if distance(o, grid) >= sum(n // 2 for n in grid) - NEARER]
    rest = offsets[len(direct) :]
    far_half = rest[0::2]
    near_half = rest[1::2]
    arrivals = slabs - 1 + len(direct)
    lane = lax.broadcasted_iota(jnp.int32, (1, LANES), 1)

    def shifted(offset):
        there, place, scale = 0, slab, slabs
        for o, n in zip(offset, grid):
            scale //= n
            at = place // scale
            place = place - at * scale
            at = at + o
            there = there + jnp.where(at >= n, at - n, jnp.where(at < 0, at + n, at)) * scale
        return there

    def send(step, source, slot, there, core):
        pltpu.make_async_remote_copy(
            source, parts.at[step, slot], r_send.at[step], r_recv.at[step],
            device_id=(there, core), device_id_type=MESH).start()

    def newton(step, level):
        @pl.when(step > 0)
        def _():
            center = jnp.broadcast_to(beta * level, (8, LANES))

            def body(i, carry):
                total, bend = carry
                at = pl.ds(pl.multiple_of(i * 8, 8), 8)
                for layer in range(depth):
                    tangents = [jnp.tanh(coded[layer, at, pl.ds(c * LANES, LANES)] - center) for c in range(cols // LANES)]
                    total = tuple(a + t for a, t in zip(total, tangents))
                    bend = tuple(a + (1.0 - t * t) for a, t in zip(bend, tangents))
                return total, bend

            zero = (jnp.zeros((8, LANES), jnp.float32),) * (cols // LANES)
            total, bend = lax.fori_loop(0, rows // 8, body, (zero, zero), unroll=6)
            acc[0] = tree(total)
            acc[1] = tree(bend)

        total = jnp.sum(acc[0], axis=0, keepdims=True)
        bend = jnp.sum(acc[1], axis=0, keepdims=True)
        total = total + pltpu.roll(total, HALF, 1)
        bend = bend + pltpu.roll(bend, HALF, 1)
        pair[step, 0] = jnp.where(lane < HALF, total, bend)
        swap = pltpu.make_async_remote_copy(
            pair.at[step, 0], pair.at[step, 1], p_send.at[step], p_recv.at[step],
            device_id=(slab, sibling), device_id_type=MESH)
        swap.start()
        for offset in direct:
            there = shifted(offset)
            for core in range(pencils):
                send(step, pair.at[step, 0], pencil * slabs + slab, there, core)
        swap.wait_recv()
        parts[step, slab] = pair[step, 0] + pair[step, 1]

        for here, chips in ((pencils - 1, far_half), (0, near_half)):
            @pl.when(pencil == here)
            def _():
                for offset in chips:
                    there = shifted(offset)
                    for core in range(pencils):
                        send(step, parts.at[step, slab], slab, there, core)

        @pl.when(step == 0)
        def _():
            @pl.loop(0, steps)
            def _(k):
                @pl.when(has_above)
                def _():
                    up_copy(k).wait_send()

                @pl.when(has_below)
                def _():
                    down_copy(k).wait_send()

            own_halo.wait_send()

            @pl.when(has_below)
            def _():
                below_halo.wait_send()

            @pl.when(has_above)
            def _():
                above_halo.wait_send()

        most = parts.at[step, pl.ds(0, arrivals)]
        pltpu.make_async_copy(most, most, r_recv.at[step]).wait()
        both = tree([parts[step, i] + parts[step, slabs + i] for i in range(slabs)])
        volume = 0.5 * (cells + jnp.sum(jnp.where(lane < HALF, both, 0.0), axis=1, keepdims=True))
        slope = cells + 0.5 * beta * jnp.sum(jnp.where(lane < HALF, 0.0, both), axis=1, keepdims=True)
        return level + (volume - fraction_ref[0] * cells) / slope

    level = lax.fori_loop(0, ITERS, newton, jnp.full((1, LANES), 0.5, jnp.float32))
    level_out[0:1] = level
    level_out[1:2] = beta * level

    for step in range(ITERS):
        pltpu.make_async_copy(pair.at[step, 0], pair.at[step, 0], p_send.at[step]).wait()

    for here, chips in ((pencils - 1, far_half), (0, near_half)):
        @pl.when(pencil == here)
        def _():
            for step in range(ITERS):
                most = parts.at[step, pl.ds(0, len(direct) + len(chips))]
                for core in range(pencils):
                    pltpu.make_async_copy(most, most, r_send.at[step]).wait()


def project(coded, level, physical, threshold, held, level_held, sems, level_sem):
    depth, rows, cols = coded.shape
    center = jnp.broadcast_to(level[1:2], (8, LANES))
    level_held[0] = jnp.max(level[0:1])
    level_copy = pltpu.make_async_copy(level_held, threshold, level_sem)
    level_copy.start()
    copies = []
    for layer in range(depth):
        @pl.loop(0, rows // 8, unroll=16)
        def _(i):
            at = pl.ds(pl.multiple_of(i * 8, 8), 8)
            for c in range(0, cols, LANES):
                held[layer, at, pl.ds(c, LANES)] = 0.5 * (1.0 + jnp.tanh(coded[layer, at, pl.ds(c, LANES)] - center))

        copies.append(pltpu.make_async_copy(held.at[layer], physical.at[layer], sems.at[layer]))
        copies[-1].start()
    for copy in copies:
        copy.wait()
    level_copy.wait()


def solution(mesh):
    slabs, pencils = mesh.shape["slab"], mesh.shape["pencil"]
    grid = GRID if math.prod(GRID) == slabs else (slabs,)

    def local(density, cell_kind, sharpness, fraction):
        depth, rows, cols = density.shape
        steps = rows // CHUNK
        wide = rows + 2 * PAD
        coded, level = pl.pallas_call(
            functools.partial(kernel, slabs, pencils, grid),
            out_shape=(jax.ShapeDtypeStruct(density.shape, jnp.float32), jax.ShapeDtypeStruct((2, LANES), jnp.float32)),
            in_specs=[pl.BlockSpec(memory_space=pltpu.HBM)] * 4,
            out_specs=(pl.BlockSpec(memory_space=pltpu.VMEM), pl.BlockSpec(memory_space=pltpu.VMEM)),
            scratch_shapes=[
                pltpu.VMEM((depth, wide, cols), jnp.float32),
                pltpu.VMEM((RADIUS, wide, cols), jnp.float32),
                pltpu.VMEM((RADIUS, wide, cols), jnp.float32),
                pltpu.VMEM((depth, rows, cols), jnp.int32),
                pltpu.VMEM((depth, wide, cols), jnp.float32),
                pltpu.VMEM((cols, cols), jnp.bfloat16),
                pltpu.VMEM((2, 8, LANES), jnp.float32),
                pltpu.VMEM((ITERS, 2, 1, LANES), jnp.float32),
                pltpu.VMEM((ITERS, 2 * slabs, 1, LANES), jnp.float32),
                pltpu.SMEM((1,), jnp.float32),
                pltpu.SMEM((1,), jnp.float32),
                pltpu.SemaphoreType.DMA((steps,)),
                pltpu.SemaphoreType.DMA((steps,)),
                pltpu.SemaphoreType.DMA((steps,)),
                pltpu.SemaphoreType.DMA((steps,)),
                pltpu.SemaphoreType.DMA((3,)),
                pltpu.SemaphoreType.DMA((3,)),
                pltpu.SemaphoreType.DMA((4,)),
                pltpu.SemaphoreType.DMA((ITERS,)),
                pltpu.SemaphoreType.DMA((ITERS,)),
                pltpu.SemaphoreType.DMA((ITERS,)),
                pltpu.SemaphoreType.DMA((ITERS,)),
                pltpu.SemaphoreType.REGULAR((max((slabs - 1).bit_length() - 1, 1),)),
            ],
            compiler_params=pltpu.CompilerParams(
                collective_id=0, has_side_effects=True, vmem_limit_bytes=49 * 1024 * 1024),
        )(sharpness, fraction, density, cell_kind)
        return pl.pallas_call(
            project,
            out_shape=(jax.ShapeDtypeStruct(density.shape, jnp.float32), jax.ShapeDtypeStruct((1,), jnp.float32)),
            in_specs=[pl.BlockSpec(memory_space=pltpu.VMEM)] * 2,
            out_specs=(pl.BlockSpec(memory_space=pltpu.HBM), pl.BlockSpec(memory_space=pltpu.HBM)),
            scratch_shapes=[
                pltpu.VMEM(density.shape, jnp.float32),
                pltpu.SMEM((1,), jnp.float32),
                pltpu.SemaphoreType.DMA((depth,)),
                pltpu.SemaphoreType.DMA,
            ],
            compiler_params=pltpu.CompilerParams(vmem_limit_bytes=8 * 1024 * 1024),
        )(coded, level)

    in_specs = (P("slab", "pencil", None), P("slab", "pencil", None), P(), P())
    out_specs = (P("slab", "pencil", None), P())
    return jax.shard_map(local, mesh=mesh, in_specs=in_specs, out_specs=out_specs, check_vma=False)
```

```python
import functools
import itertools
import math

import jax
import jax.numpy as jnp
from jax import lax
from jax.experimental import pallas as pl
from jax.experimental.pallas import tpu as pltpu
from jax.sharding import PartitionSpec as P

RADIUS = 5
ITERS = 3
CHUNK = 16
PAD = 8
LANES = 128
HALF = 64
NEARER = 2
WAIT = 5
GRID = (4, 8, 4)
FAR = 1.0e6
MESH = pl.DeviceIdType.MESH


def box(values):
    pairs = [a + b for a, b in zip(values[:-1], values[1:])]
    return [pairs[k] + pairs[k + 2] + pairs[k + 4] for k in range(len(values) - RADIUS)]


def triangle(k):
    k = jnp.maximum(k, 0)
    return (k * (k + 1)) // 2


def coverage(index, whole):
    full = (RADIUS + 1) * (RADIUS + 1)
    return (full - triangle(RADIUS - index) - triangle(RADIUS + 1 + index - whole)).astype(jnp.float32)


def split(x):
    high = x.astype(jnp.bfloat16)
    return high, (x - high.astype(jnp.float32)).astype(jnp.bfloat16)


def band(shape, shift):
    row = lax.broadcasted_iota(jnp.int32, shape, 0)
    col = lax.broadcasted_iota(jnp.int32, shape, 1)
    return jnp.maximum(RADIUS + 1 - jnp.abs(col - shift - row), 0).astype(jnp.float32).astype(jnp.bfloat16)


def tree(parts):
    parts = list(parts)
    while len(parts) > 1:
        parts = [sum(parts[i : i + 2][1:], parts[i]) for i in range(0, len(parts), 2)]
    return parts[0]


def folded(x):
    return tree(x[i : i + 8, j : j + LANES] for i in range(0, x.shape[0], 8) for j in range(0, x.shape[1], LANES))


def distance(offset, sizes):
    return sum(min(o, n - o) for o, n in zip(offset, sizes))


def kernel(slabs, pencils, grid, beta_in, fraction_in, density, kind, coded, level_out, own, below, above, kinds,
           along_z, x_band, acc, pair, parts, beta_ref, fraction_ref, u_send, u_recv, d_send, d_recv, h_send, h_recv,
           local_sem, p_send, p_recv, r_send, r_recv, known):
    depth, rows, cols = density.shape
    steps = rows // CHUNK
    reach = max((slabs - 1).bit_length() - 1, 1)
    slab = lax.axis_index("slab")
    pencil = lax.axis_index("pencil")
    first = pencil == 0
    devices = slabs * pencils

    barrier = pltpu.get_barrier_semaphore()

    def around(step):
        there = slab + (step if step > 0 else slabs + step)
        return there - jnp.where(there >= slabs, slabs, 0)

    for step in (1, -1):
        pl.semaphore_signal(barrier, inc=1, device_id=(around(step), pencil), device_id_type=MESH)
    pl.semaphore_signal(barrier, inc=1, device_id=(slab, 1 - pencil), device_id_type=MESH)

    def spread(j):
        for step in (1 << j, -(1 << j)):
            pl.semaphore_signal(known.at[j], inc=1, device_id=(around(step), pencil), device_id_type=MESH)

    has_above = slab + 1 < slabs
    has_below = slab > 0
    upper = jnp.minimum(slab + 1, slabs - 1)
    lower = jnp.maximum(slab - 1, 0)
    sibling = 1 - pencil
    halo = pl.multiple_of(jnp.where(first, PAD + rows, 0), 8)
    edge = pl.multiple_of(jnp.where(first, 0, PAD + rows), 8)
    there = pl.multiple_of(jnp.where(first, 0, PAD + rows), 8)
    mine = pl.multiple_of(jnp.where(first, rows, PAD), 8)

    def row_of(k):
        return pl.multiple_of(jnp.where(first, steps - 1 - k, k) * CHUNK, CHUNK)

    def up_copy(k):
        r = row_of(k)
        return pltpu.make_async_remote_copy(
            density.at[pl.ds(depth - RADIUS, RADIUS), pl.ds(r, CHUNK), :], below.at[:, pl.ds(r + PAD, CHUNK), :],
            u_send.at[k], u_recv.at[k], device_id=(upper, pencil), device_id_type=MESH)

    def down_copy(k):
        r = row_of(k)
        return pltpu.make_async_remote_copy(
            density.at[pl.ds(0, RADIUS), pl.ds(r, CHUNK), :], above.at[:, pl.ds(r + PAD, CHUNK), :],
            d_send.at[k], d_recv.at[k], device_id=(lower, pencil), device_id_type=MESH)

    def halo_copy(index, src, dst):
        return pltpu.make_async_remote_copy(
            src, dst, h_send.at[index], h_recv.at[index], device_id=(slab, sibling), device_id_type=MESH)

    own_row = pl.multiple_of(jnp.where(first, rows - PAD, 0), 8)
    own_halo = halo_copy(0, density.at[:, pl.ds(own_row, PAD), :], own.at[:, pl.ds(there, PAD), :])
    below_halo = halo_copy(1, below.at[:, pl.ds(mine, PAD), :], below.at[:, pl.ds(there, PAD), :])
    above_halo = halo_copy(2, above.at[:, pl.ds(mine, PAD), :], above.at[:, pl.ds(there, PAD), :])
    own_load = pltpu.make_async_copy(density, own.at[:, pl.ds(PAD, rows), :], local_sem.at[0])
    kind_load = pltpu.make_async_copy(kind, kinds, local_sem.at[1])
    beta_load = pltpu.make_async_copy(beta_in, beta_ref, local_sem.at[2])
    fraction_load = pltpu.make_async_copy(fraction_in, fraction_ref, local_sem.at[3])

    own_load.start()
    kind_load.start()
    beta_load.start()
    fraction_load.start()
    pl.semaphore_wait(barrier, 3)

    def send_chunk(k):
        @pl.when(has_above)
        def _():
            up_copy(k).start()

        @pl.when(has_below)
        def _():
            down_copy(k).start()

    pl.loop(0, steps)(send_chunk)
    parts[:, slabs:] = jnp.zeros((ITERS, slabs, 1, LANES), jnp.float32)
    own_halo.start()

    x_band[...] = band((cols, cols), 0)
    acc[...] = jnp.zeros_like(acc)
    along_z[:, pl.ds(edge, PAD), :] = jnp.zeros((depth, PAD, cols), jnp.float32)

    @pl.when(jnp.logical_not(has_below))
    def _():
        @pl.loop(0, RADIUS)
        def _(k):
            below[k] = jnp.zeros(below.shape[1:], jnp.float32)

    @pl.when(jnp.logical_not(has_above))
    def _():
        @pl.loop(0, RADIUS)
        def _(k):
            above[k] = jnp.zeros(above.shape[1:], jnp.float32)

    beta_load.wait()
    fraction_load.wait()
    beta = beta_ref[0]

    def filter_z(start, count):
        for r in range(0, count, 8):
            for c in range(0, cols, LANES):
                at = (pl.ds(pl.multiple_of(start + r, 8), 8), pl.ds(c, LANES))
                values = [below[m, at[0], at[1]] for m in range(RADIUS)]
                values += [own[i, at[0], at[1]] for i in range(depth)]
                values += [above[i, at[0], at[1]] for i in range(RADIUS)]
                for i, out in enumerate(box(box(values))):
                    along_z[i, at[0], at[1]] = out

    def filter_yx(j):
        r = row_of(j)
        y_band = band((CHUNK, CHUNK + 2 * PAD), PAD)
        pieces = []
        for layer in range(depth):
            high, low = split(along_z[layer, pl.ds(r, CHUNK + 2 * PAD), :])
            pieces.append(jnp.dot(y_band, high, preferred_element_type=jnp.float32)
                          + jnp.dot(y_band, low, preferred_element_type=jnp.float32))
        high, low = split(jnp.concatenate(pieces, axis=0))
        smoothed = (jnp.dot(high, x_band[...], preferred_element_type=jnp.float32)
                    + jnp.dot(low, x_band[...], preferred_element_type=jnp.float32))
        row = lax.broadcasted_iota(jnp.int32, (CHUNK, cols), 0) + (pencil * rows + r)
        col = lax.broadcasted_iota(jnp.int32, (CHUNK, cols), 1)
        cover_y = coverage(row, rows * pencils)
        cover_x = coverage(col, cols)
        for layer in range(depth):
            depth_index = jnp.full((1, cols), slab * depth + layer, jnp.int32)
            cover = coverage(depth_index, slabs * depth) * cover_y * cover_x
            filtered = smoothed[layer * CHUNK : (layer + 1) * CHUNK] / cover
            which = kinds[layer, pl.ds(r, CHUNK), :]
            value = jnp.where(which == 0, beta * filtered, jnp.where(which == 2, FAR, -FAR))
            coded[layer, pl.ds(r, CHUNK), :] = value
            tangent = jnp.tanh(value - 0.5 * beta)
            acc[0] += folded(tangent)
            acc[1] += folded(1.0 - tangent * tangent)

    @pl.loop(0, steps + 1)
    def _(k):
        @pl.when(k < steps)
        def _():
            @pl.when(has_below)
            def _():
                up_copy(k).wait_recv()

                @pl.when(k == 0)
                def _():
                    below_halo.start()

            @pl.when(has_above)
            def _():
                down_copy(k).wait_recv()

                @pl.when(k == 0)
                def _():
                    above_halo.start()

            @pl.when(k == 0)
            def _():
                own_load.wait()
                kind_load.wait()

            filter_z(row_of(k) + PAD, CHUNK)

        @pl.when(k == 1)
        def _():
            own_halo.wait_recv()

            @pl.when(has_below)
            def _():
                below_halo.wait_recv()

            @pl.when(has_above)
            def _():
                above_halo.wait_recv()

            filter_z(halo, PAD)

        @pl.when(k >= 1)
        def _():
            filter_yx(k - 1)

        @pl.when(k == WAIT - 1)
        def _():
            spread(0)

        for j in range(reach):
            @pl.when(k == WAIT + j)
            def _():
                pl.semaphore_wait(known.at[j], 2)
                if j + 1 < reach:
                    spread(j + 1)

    cells = float(devices) * float(depth * rows * cols)
    offsets = [o for o in itertools.product(*(range(n) for n in grid)) if any(o)]
    offsets.sort(key=lambda o: -distance(o, grid))
    direct = [o for o in offsets if distance(o, grid) >= sum(n // 2 for n in grid) - NEARER]
    rest = offsets[len(direct) :]
    far_half = rest[0::2]
    near_half = rest[1::2]
    arrivals = slabs - 1 + len(direct)
    lane = lax.broadcasted_iota(jnp.int32, (1, LANES), 1)

    def shifted(offset):
        there, place, scale = 0, slab, slabs
        for o, n in zip(offset, grid):
            scale //= n
            at = place // scale
            place = place - at * scale
            at = at + o
            there = there + jnp.where(at >= n, at - n, jnp.where(at < 0, at + n, at)) * scale
        return there

    def send(step, source, slot, there, core):
        pltpu.make_async_remote_copy(
            source, parts.at[step, slot], r_send.at[step], r_recv.at[step],
            device_id=(there, core), device_id_type=MESH).start()

    def newton(step, level):
        @pl.when(step > 0)
        def _():
            center = jnp.broadcast_to(beta * level, (8, LANES))

            def body(i, carry):
                total, bend = carry
                at = pl.ds(pl.multiple_of(i * 8, 8), 8)
                for layer in range(depth):
                    tangents = [jnp.tanh(coded[layer, at, pl.ds(c * LANES, LANES)] - center) for c in range(cols // LANES)]
                    total = tuple(a + t for a, t in zip(total, tangents))
                    bend = tuple(a + (1.0 - t * t) for a, t in zip(bend, tangents))
                return total, bend

            zero = (jnp.zeros((8, LANES), jnp.float32),) * (cols // LANES)
            total, bend = lax.fori_loop(0, rows // 8, body, (zero, zero), unroll=6)
            acc[0] = tree(total)
            acc[1] = tree(bend)

        total = jnp.sum(acc[0], axis=0, keepdims=True)
        bend = jnp.sum(acc[1], axis=0, keepdims=True)
        total = total + pltpu.roll(total, HALF, 1)
        bend = bend + pltpu.roll(bend, HALF, 1)
        pair[step, 0] = jnp.where(lane < HALF, total, bend)
        swap = pltpu.make_async_remote_copy(
            pair.at[step, 0], pair.at[step, 1], p_send.at[step], p_recv.at[step],
            device_id=(slab, sibling), device_id_type=MESH)
        swap.start()
        for offset in direct:
            there = shifted(offset)
            for core in range(pencils):
                send(step, pair.at[step, 0], pencil * slabs + slab, there, core)
        swap.wait_recv()
        parts[step, slab] = pair[step, 0] + pair[step, 1]

        for here, chips in ((pencils - 1, far_half), (0, near_half)):
            @pl.when(pencil == here)
            def _():
                for offset in chips:
                    there = shifted(offset)
                    for core in range(pencils):
                        send(step, parts.at[step, slab], slab, there, core)

        @pl.when(step == 0)
        def _():
            @pl.loop(0, steps)
            def _(k):
                @pl.when(has_above)
                def _():
                    up_copy(k).wait_send()

                @pl.when(has_below)
                def _():
                    down_copy(k).wait_send()

            own_halo.wait_send()

            @pl.when(has_below)
            def _():
                below_halo.wait_send()

            @pl.when(has_above)
            def _():
                above_halo.wait_send()

        most = parts.at[step, pl.ds(0, arrivals)]
        pltpu.make_async_copy(most, most, r_recv.at[step]).wait()
        both = tree([parts[step, i] + parts[step, slabs + i] for i in range(slabs)])
        volume = 0.5 * (cells + jnp.sum(jnp.where(lane < HALF, both, 0.0), axis=1, keepdims=True))
        slope = cells + 0.5 * beta * jnp.sum(jnp.where(lane < HALF, 0.0, both), axis=1, keepdims=True)
        return level + (volume - fraction_ref[0] * cells) / slope

    level = lax.fori_loop(0, ITERS, newton, jnp.full((1, LANES), 0.5, jnp.float32))
    level_out[0:1] = level
    level_out[1:2] = beta * level

    for step in range(ITERS):
        pltpu.make_async_copy(pair.at[step, 0], pair.at[step, 0], p_send.at[step]).wait()

    for here, chips in ((pencils - 1, far_half), (0, near_half)):
        @pl.when(pencil == here)
        def _():
            for step in range(ITERS):
                most = parts.at[step, pl.ds(0, len(direct) + len(chips))]
                for core in range(pencils):
                    pltpu.make_async_copy(most, most, r_send.at[step]).wait()


def project(coded, level, physical, threshold, held, level_held, sems, level_sem):
    depth, rows, cols = coded.shape
    center = jnp.broadcast_to(level[1:2], (8, LANES))
    level_held[0] = jnp.max(level[0:1])
    level_copy = pltpu.make_async_copy(level_held, threshold, level_sem)
    level_copy.start()
    copies = []
    half = rows // 2
    for piece in range(2 * depth):
        layer, start = piece // 2, piece % 2 * half

        @pl.loop(0, half // 8, unroll=12)
        def _(i):
            at = pl.ds(pl.multiple_of(start + i * 8, 8), 8)
            for c in range(0, cols, LANES):
                held[layer, at, pl.ds(c, LANES)] = 0.5 * (1.0 + jnp.tanh(coded[layer, at, pl.ds(c, LANES)] - center))

        band_rows = pl.ds(start, half)
        copies.append(pltpu.make_async_copy(held.at[layer, band_rows], physical.at[layer, band_rows], sems.at[piece]))
        copies[-1].start()
    for copy in copies:
        copy.wait()
    level_copy.wait()


def solution(mesh):
    slabs, pencils = mesh.shape["slab"], mesh.shape["pencil"]
    grid = GRID if math.prod(GRID) == slabs else (slabs,)

    def local(density, cell_kind, sharpness, fraction):
        depth, rows, cols = density.shape
        steps = rows // CHUNK
        wide = rows + 2 * PAD
        coded, level = pl.pallas_call(
            functools.partial(kernel, slabs, pencils, grid),
            out_shape=(jax.ShapeDtypeStruct(density.shape, jnp.float32), jax.ShapeDtypeStruct((2, LANES), jnp.float32)),
            in_specs=[pl.BlockSpec(memory_space=pltpu.HBM)] * 4,
            out_specs=(pl.BlockSpec(memory_space=pltpu.VMEM), pl.BlockSpec(memory_space=pltpu.VMEM)),
            scratch_shapes=[
                pltpu.VMEM((depth, wide, cols), jnp.float32),
                pltpu.VMEM((RADIUS, wide, cols), jnp.float32),
                pltpu.VMEM((RADIUS, wide, cols), jnp.float32),
                pltpu.VMEM((depth, rows, cols), jnp.int32),
                pltpu.VMEM((depth, wide, cols), jnp.float32),
                pltpu.VMEM((cols, cols), jnp.bfloat16),
                pltpu.VMEM((2, 8, LANES), jnp.float32),
                pltpu.VMEM((ITERS, 2, 1, LANES), jnp.float32),
                pltpu.VMEM((ITERS, 2 * slabs, 1, LANES), jnp.float32),
                pltpu.SMEM((1,), jnp.float32),
                pltpu.SMEM((1,), jnp.float32),
                pltpu.SemaphoreType.DMA((steps,)),
                pltpu.SemaphoreType.DMA((steps,)),
                pltpu.SemaphoreType.DMA((steps,)),
                pltpu.SemaphoreType.DMA((steps,)),
                pltpu.SemaphoreType.DMA((3,)),
                pltpu.SemaphoreType.DMA((3,)),
                pltpu.SemaphoreType.DMA((4,)),
                pltpu.SemaphoreType.DMA((ITERS,)),
                pltpu.SemaphoreType.DMA((ITERS,)),
                pltpu.SemaphoreType.DMA((ITERS,)),
                pltpu.SemaphoreType.DMA((ITERS,)),
                pltpu.SemaphoreType.REGULAR((max((slabs - 1).bit_length() - 1, 1),)),
            ],
            compiler_params=pltpu.CompilerParams(
                collective_id=0, has_side_effects=True, vmem_limit_bytes=49 * 1024 * 1024),
        )(sharpness, fraction, density, cell_kind)
        return pl.pallas_call(
            project,
            out_shape=(jax.ShapeDtypeStruct(density.shape, jnp.float32), jax.ShapeDtypeStruct((1,), jnp.float32)),
            in_specs=[pl.BlockSpec(memory_space=pltpu.VMEM)] * 2,
            out_specs=(pl.BlockSpec(memory_space=pltpu.HBM), pl.BlockSpec(memory_space=pltpu.HBM)),
            scratch_shapes=[
                pltpu.VMEM(density.shape, jnp.float32),
                pltpu.SMEM((1,), jnp.float32),
                pltpu.SemaphoreType.DMA((2 * depth,)),
                pltpu.SemaphoreType.DMA,
            ],
            compiler_params=pltpu.CompilerParams(vmem_limit_bytes=8 * 1024 * 1024),
        )(coded, level)

    in_specs = (P("slab", "pencil", None), P("slab", "pencil", None), P(), P())
    out_specs = (P("slab", "pencil", None), P())
    return jax.shard_map(local, mesh=mesh, in_specs=in_specs, out_specs=out_specs, check_vma=False)
```
